32 devices in a mesh: gx: 8 (over z, core), gz: 4 (over y, x).
Axes of the slice: x: 2, y: 2, z: 4, core: 2. Of those that a mesh axis runs over, the one named last changes fastest.
Arguments:
- view_index: int32 [1], replicated, may hold values from 0 to 5
- psf_taps: float32 [6, 3, 31], replicated, may hold values from 0.1 to 1
- extents: int32 [6, 3], replicated, may hold values from 4 to 15
- estimate: float32 [16, 256, 1024], P(None, 'gz', 'gx'), may hold values from 0.5 to 2
- measured: float32 [16, 256, 1024], P(None, 'gz', 'gx'), may hold values from 0.25 to 4
Outputs:
- upsampled: float32 [16, 1024, 1024], P('gz', None, 'gx')
The draws below stay inside these ranges and needn't reach their ends.
All inputs are finite; a program needn't handle non-finite values.
Results may differ from the reference program's by a relative error of at most 0.004.
Values may be sent and summed in bfloat16 or wider, within the bound.
A program may use at most 64 MiB of HBM per device.

```python
import math
import jax
import jax.numpy as jnp
from jax import lax

Y = 16
HALF = 15
TAPS = 31
VIEWS = 6
UP = 4
NX = 1024
NZ = 256


def with_ends(result, own_key, low, largest):
    spot = [jax.random.randint(jax.random.fold_in(own_key, axis), (), 0, length) for axis, length in enumerate(result.shape)]
    widest = result.shape.index(max(result.shape))
    next_to = spot[:widest] + [(spot[widest] + 1) % result.shape[widest]] + spot[widest + 1:]
    return result.at[tuple(spot)].set(low).at[tuple(next_to)].set(largest)


def block_levels(stream_key, dims, split, low, top_value):
    loudness, own = 1.0, jax.random.fold_in(stream_key, 6)
    for dim, blocks in split:
        steps = jnp.exp(jax.random.uniform(jax.random.fold_in(own, dim), (blocks,), jnp.float32, low / len(split), top_value / len(split)))
        loudness = loudness * jnp.repeat(steps, dims[dim] // blocks).reshape([-1 if axis == dim else 1 for axis in range(len(dims))])
    return loudness


def setup_inputs(seed: int = 0) -> dict:
    seeds = jax.random.split(jax.random.key(seed), 6)
    return {
        "view_index": jax.random.randint(seeds[0], (1,), 0, VIEWS).astype(jnp.int32),
        "psf_taps": jnp.clip(jnp.exp(jax.random.uniform(seeds[1], (VIEWS, 3, TAPS), jnp.float32, math.log(0.1), math.log(1.0))), 0.1, 1.0),
        "extents": with_ends(jax.random.randint(seeds[2], (VIEWS, 3), 4, HALF + 1), jax.random.fold_in(seeds[2], 1), 4, HALF).astype(jnp.int32),
        "estimate": jnp.clip(jnp.exp(math.log(2.0) - 1.3862944 * jax.random.uniform(seeds[3], (Y, NZ, NX), jnp.float32) ** block_levels(seeds[3], (Y, NZ, NX), ((1, 4), (2, 8)), -0.2, 0.2)), 0.5, 2.0),
        "measured": jnp.clip(jnp.exp(math.log(4.0) - 2.7725887 * jax.random.uniform(seeds[4], (Y, NZ, NX), jnp.float32) ** block_levels(seeds[4], (Y, NZ, NX), ((1, 4), (2, 8)), -0.2, 0.2)), 0.25, 4.0),
    }


def pick_kernels(view_index, psf_taps, extents):
    chosen = view_index[0]
    offsets = jnp.arange(TAPS, dtype=jnp.int32) - HALF
    kernels = []
    for axis_id in range(3):
        unnormalized_taps = psf_taps[chosen, axis_id] * (jnp.abs(offsets) <= extents[chosen, axis_id]).astype(jnp.float32)
        kernels.append(unnormalized_taps / jnp.sum(unnormalized_taps))
    return kernels


def smear(volume, kernel, axis_dim):
    length = volume.shape[axis_dim]
    pad_widths = [(0, 0), (0, 0), (0, 0)]
    pad_widths[axis_dim] = (HALF, HALF)
    padded = jnp.pad(volume, pad_widths)
    total = jnp.zeros_like(volume)
    for tap_index in range(TAPS):
        total = total + kernel[tap_index] * lax.slice_in_dim(padded, tap_index, tap_index + length, axis=axis_dim)
    return total


def blur(volume, kernels):
    section_one = smear(volume, kernels[0], 2)
    section_two = smear(section_one, kernels[1], 0)
    return smear(section_two, kernels[2], 1)


def build_table(first_row, count_of_rows, length):
    row_ids = first_row + jnp.arange(count_of_rows, dtype=jnp.int32)[:, None]
    column_numbers = jnp.arange(length, dtype=jnp.int32)[None, :]
    offset_units = jnp.mod(row_ids - UP * column_numbers, UP * length)
    sine_part = jnp.sin(jnp.pi * jnp.mod(offset_units, 2 * UP).astype(jnp.float32) / UP)
    tangent_part = length * jnp.tan(jnp.pi * offset_units.astype(jnp.float32) / (UP * length))
    on_grid = jnp.mod(offset_units, UP) == 0
    guarded_denominator = jnp.where(on_grid, jnp.float32(1.0), tangent_part)
    entries = jnp.where(on_grid, jnp.where(offset_units == 0, jnp.float32(1.0), jnp.float32(0.0)), sine_part / guarded_denominator)
    return entries.astype(jnp.bfloat16)


def reference(view_index, psf_taps, extents, estimate, measured):
    kernels = pick_kernels(view_index, psf_taps, extents)
    blurred = blur(estimate, kernels)
    quotient = measured / blurred
    correction = blur(quotient, [kernel[::-1] for kernel in kernels])
    rounded = (estimate * correction).astype(jnp.bfloat16)
    full_table = build_table(0, UP * NZ, NZ)

    def per_plane(slab_plane):
        return jnp.dot(full_table, slab_plane, preferred_element_type=jnp.float32)

    return lax.map(per_plane, rounded)
```

```python
import jax
import jax.numpy as jnp
from jax import lax
from jax.sharding import PartitionSpec as P

UP = 4
BF = jnp.bfloat16


def pick_kernels(view_index, psf_taps, extents):
    half = (psf_taps.shape[2] - 1) // 2
    selector = (jnp.arange(psf_taps.shape[0], dtype=jnp.int32) == view_index[0]).astype(jnp.float32)
    picked = jnp.sum(psf_taps * selector[:, None, None], axis=0)
    reach = jnp.sum(extents.astype(jnp.float32) * selector[:, None], axis=0)
    offsets = (jnp.arange(psf_taps.shape[2], dtype=jnp.int32) - half).astype(jnp.float32)
    raw = picked * (jnp.abs(offsets)[None, :] <= reach[:, None]).astype(jnp.float32)
    return raw / jnp.sum(raw, axis=1, keepdims=True)


def band(kernel, rows, cols, lead, sign):
    half = (kernel.shape[0] - 1) // 2
    i = lax.broadcasted_iota(jnp.int32, (rows, cols), 0) - lead
    j = lax.broadcasted_iota(jnp.int32, (rows, cols), 1)
    t = sign * (i - j) + half
    total = jnp.zeros((rows, cols), jnp.float32)
    for tap in range(kernel.shape[0]):
        total = jnp.where(t == tap, kernel[tap], total)
    return total.astype(BF)


def extended(cells, axis, dim, width):
    count = lax.axis_size(axis)
    ends = count - 1
    head = lax.slice_in_dim(cells, 0, width, axis=dim)
    tail = lax.slice_in_dim(cells, cells.shape[dim] - width, cells.shape[dim], axis=dim)
    return jnp.concatenate(
        [
            lax.ppermute(tail, axis, [(i, i + 1) for i in range(ends)]),
            cells,
            lax.ppermute(head, axis, [(i + 1, i) for i in range(ends)]),
        ],
        axis=dim,
    )


def blur(volume, kernels, sign):
    y, z, x = volume.shape
    half = (kernels.shape[1] - 1) // 2
    lead = half + 1
    wide = extended(volume.astype(BF), "gx", 2, lead)
    kx = band(kernels[0], x + 2 * lead, x, lead, sign)
    ky = band(kernels[1], y, y, 0, sign)
    kz = band(kernels[2], z + 2 * lead, z, lead, sign)
    one = jnp.einsum("yzi,ij->yzj", wide, kx, preferred_element_type=jnp.float32).astype(BF)
    two = jnp.einsum("yzi,yj->jzi", one, ky, preferred_element_type=jnp.float32).astype(BF)
    tall = extended(two, "gz", 1, lead)
    return jnp.einsum("zj,yzi->yji", kz, tall, preferred_element_type=jnp.float32)


def build_table(length):
    rows = UP * length
    row_ids = lax.broadcasted_iota(jnp.int32, (rows, length), 0)
    cols = lax.broadcasted_iota(jnp.int32, (rows, length), 1)
    units = jnp.mod(row_ids - UP * cols, rows)
    sine = jnp.sin(jnp.pi * jnp.mod(units, 2 * UP).astype(jnp.float32) / UP)
    tangent = length * jnp.tan(jnp.pi * units.astype(jnp.float32) / rows)
    on_grid = jnp.mod(units, UP) == 0
    guarded = jnp.where(on_grid, jnp.float32(1.0), tangent)
    hit = jnp.where(units == 0, jnp.float32(1.0), jnp.float32(0.0))
    return jnp.where(on_grid, hit, sine / guarded).astype(BF)


def on_device(view_index, psf_taps, extents, estimate, measured):
    kernels = pick_kernels(view_index, psf_taps, extents)
    blurred = blur(estimate, kernels, 1)
    correction = blur(measured / blurred, kernels, -1)
    rounded = (estimate * correction).astype(BF)
    lines = lax.all_to_all(rounded, "gz", split_axis=0, concat_axis=1, tiled=True)
    table = build_table(lines.shape[1])
    return jnp.einsum("mn,ynx->ymx", table, lines, preferred_element_type=jnp.float32)


def solution(mesh):
    return jax.shard_map(
        on_device,
        mesh=mesh,
        in_specs=(P(), P(), P(), P(None, "gz", "gx"), P(None, "gz", "gx")),
        out_specs=P("gz", None, "gx"),
        check_vma=False,
    )
```
